32 devices in a mesh: seq: 4 (over x, core), head: 8 (over z, y).
Axes of the slice: x: 2, y: 2, z: 4, core: 2. Of those that a mesh axis runs over, the one named last changes fastest.
Arguments:
- queries: bfloat16 [256, 4096], P('seq', 'head'), may hold values from -8 to 8
- new_keys: bfloat16 [256, 256], P('seq'), may hold values from -6 to 6
- new_values: bfloat16 [256, 256], P('seq'), may hold values from -6 to 6
- cache_keys: bfloat16 [3072, 256], P('seq'), may hold values from -8 to 8
- cache_values: bfloat16 [3072, 256], P('seq'), may hold values from -6 to 6
- positions: int32 [256], replicated, may hold values from 0 to 255, each once
- cache_len: int32 [4], replicated, may hold values from 1 to 768, 1920 in all
- out_weight: bfloat16 [4096, 16384], P('head', 'seq'), may hold values from -3.5 to 3.5
Outputs:
- output: float32 [256, 16384], P(None, 'seq')
The draws below stay inside these ranges and needn't reach their ends.
Inputs may be any that keep to these rules, and one draw needn't show every extreme that they name: A permutation of the block's positions 0 to 255. `cache_len`: entry s is the number of live slots at the start of sequence group s's 768 cache slots; later slots of that group are not attended. Some group is full.
All inputs are finite; a program needn't handle non-finite values.
Results may differ from the reference program's by a relative error of at most 0.009.
Values may be sent and summed in bfloat16 or wider, within the bound.
A program may use at most 128 MiB of HBM per device.

```python
import math
import jax
import jax.numpy as jnp
import numpy as np
from jax import lax

D = 16384
DH = 128
GQA = 16
CSTR = 768
H = 32
KVH = 2
TOKENS = 256
CACHE = 3072
N_SEQ = 4


def draw_queries(key, part):
    base = jax.random.truncated_normal(jax.random.fold_in(key, 11), -8.0, 8.0, (TOKENS, H * DH), jnp.float32)
    return base.astype(jnp.bfloat16)


def draw_cache_keys(key, part):
    base = jax.random.truncated_normal(jax.random.fold_in(key, 23), -8.0, 8.0, (CACHE, KVH * DH), jnp.float32)
    return base.astype(jnp.bfloat16)


def shard_levels(stream_key, extent, pieces, smallest, top_value):
    def one(position, shards_of):
        heights = jax.random.uniform(jax.random.fold_in(jax.random.fold_in(stream_key, 6), position), (shards_of,), jnp.float32, smallest / len(pieces), top_value / len(pieces))
        return jnp.repeat(jnp.exp(heights), extent[position] // shards_of).reshape((-1,) + (1,) * (len(extent) - position - 1))

    level = one(*pieces[0])
    for cut in pieces[1:]:
        level = level * one(*cut)
    return level


def profile(amount, total, most, slope):
    portions = [(1 << 20) // math.isqrt(grade ** slope) + 1 for grade in range(2, amount + 1)]
    spare, counts = total - most - (amount - 1), [1] * (amount - 1)
    while spare > 0:
        free = [i for i in range(amount - 1) if counts[i] < most]
        mass, left = sum([portions[i] for i in free]), spare
        for i in free:
            addition = min(most - counts[i], max(1, left * portions[i] // mass), spare)
            counts[i] = counts[i] + addition
            spare = spare - addition
    return np.array([most] + counts)


def ragged(rng, number_of, total, reach, slope):
    if number_of == 2:
        one = jax.random.randint(rng, (), max(1, total - reach), min(reach, total - 1) + 1)
        return jnp.stack([one, total - one])
    sizes = jnp.asarray(profile(number_of, total, reach, slope), jnp.int32)
    couples = (number_of - 1) // 2
    source_of, taker = sizes[1:1 + 2 * couples:2], sizes[2:2 + 2 * couples:2]
    slack = jnp.minimum(source_of - 1, reach - taker)
    passed = jax.random.randint(jax.random.fold_in(rng, 1), (couples,), 0, 1 << 20) % (slack + 1)
    sizes = sizes.at[1:1 + 2 * couples:2].set(source_of - passed).at[2:2 + 2 * couples:2].set(taker + passed)
    return sizes[jax.random.permutation(jax.random.fold_in(rng, 2), number_of)]


def normal_values(stream_key, extent, scale, bound, pieces=(), kind=jnp.bfloat16):
    drawn = jax.random.normal(stream_key, extent, jnp.float32) * scale
    if len(pieces) > 0:
        drawn = shard_levels(stream_key, extent, pieces, -0.22, 0.18) * drawn
    return jnp.clip(drawn, min=-bound, max=bound).astype(kind)


def setup_inputs(seed: int = 0) -> dict:
    key_list = jax.random.split(jax.random.key(seed), 9)
    return {
        "queries": draw_queries(jax.random.fold_in(key_list[8], 71), 0),
        "new_keys": normal_values(key_list[1], (TOKENS, KVH * DH), 1.0, 6.0, ((0, 4),)),
        "new_values": normal_values(key_list[2], (TOKENS, KVH * DH), 1.0, 6.0, ((0, 4),)),
        "cache_keys": draw_cache_keys(jax.random.fold_in(key_list[8], 71), 0),
        "cache_values": normal_values(key_list[4], (CACHE, KVH * DH), 1.0, 6.0, ((0, 4),)),
        "positions": jax.random.permutation(key_list[5], TOKENS).astype(jnp.int32),
        "cache_len": ragged(key_list[6], N_SEQ, CACHE * 5 // 8, CSTR, 2).astype(jnp.int32),
        "out_weight": normal_values(key_list[7], (H * DH, D), (H * DH * 3 // (CACHE + TOKENS)) ** -0.5, 3.5, ((0, 8), (1, 4))),
    }


def reference(queries, new_keys, new_values, cache_keys, cache_values, positions, cache_len, out_weight):
    slots = jnp.arange(CACHE, dtype=jnp.int32)
    live = (slots % CSTR) < jnp.repeat(cache_len, CSTR, total_repeat_length=CACHE)
    causal = positions[None, :] <= positions[:, None]
    shown = jnp.concatenate([jnp.broadcast_to(live[None, :], (TOKENS, CACHE)), causal], axis=1)
    all_keys = jnp.concatenate([cache_keys, new_keys], axis=0)
    all_values = jnp.concatenate([cache_values, new_values], axis=0)

    def one_head(head):
        group = head // GQA
        query = lax.dynamic_slice_in_dim(queries, (head * DH).astype(jnp.int32), DH, 1)
        key_cols = lax.dynamic_slice_in_dim(all_keys, (group * DH).astype(jnp.int32), DH, 1)
        value_cols = lax.dynamic_slice_in_dim(all_values, (group * DH).astype(jnp.int32), DH, 1)
        scores = jnp.dot(query, key_cols.T, preferred_element_type=jnp.float32) * (DH ** -0.5)
        scores = jnp.where(shown, scores, -1e30)
        peak = jnp.max(scores, axis=1, keepdims=True)
        expo = jnp.where(shown, jnp.exp(scores - peak), 0.0)
        weight_sum = jnp.sum(expo, axis=1)
        mixed = jnp.dot(expo.astype(jnp.bfloat16), value_cols, preferred_element_type=jnp.float32)
        return (mixed / weight_sum[:, None]).astype(jnp.bfloat16)

    heads = lax.map(one_head, jnp.arange(H, dtype=jnp.int32))
    attended = jnp.transpose(heads, (1, 0, 2)).reshape(TOKENS, H * DH)
    return jnp.dot(attended, out_weight, preferred_element_type=jnp.float32)
```

```python
from functools import partial

import jax
import jax.numpy as jnp
from jax import lax
from jax.experimental import pallas as pl
from jax.experimental.pallas import tpu as pltpu
from jax.sharding import PartitionSpec as P

DH = 128
GQA = 16
MESH = pl.DeviceIdType.MESH
HIDDEN = -1e30


def kernel(
    n_seq, n_head, groups,
    q_ref, ck_ref, nk_ref, cv_ref, nv_ref, pos_ref, len_ref, w_hbm,
    out_ref,
    w_ref, k_ref, v_ref, q_all, o_send, o_recv, t_send, t_recv, att,
    y_send, y_recv, z_send, z_recv, own, fin,
    w_sem, q_s, q_r, o_s, o_r, t_s, t_r, a_s, a_r,
    y_s, y_r, z_s, z_r, f_s, f_r, g_s, g_r,
):
    f32, bf16 = jnp.float32, jnp.bfloat16
    me = lax.axis_index("seq")
    head = lax.axis_index("head")
    n_out = n_head // 2
    y = lax.rem(head, 2)
    z = head // 2
    mate = z * 2 + (1 - y)
    tok, width = q_ref.shape
    heads = width // DH
    stripe = ck_ref.shape[0]
    total = n_seq * tok
    cols = w_hbm.shape[1]
    wide = cols // groups
    half = wide // 2
    rows = total // n_out

    w_copy = pltpu.make_async_copy(w_hbm, w_ref, w_sem)
    w_copy.start()

    def seq_id(d):
        return lax.rem(me + d, n_seq)

    def z_id(d):
        return lax.rem(z + d, n_out)

    barrier = pltpu.get_barrier_semaphore()
    for d in range(1, n_seq):
        pl.semaphore_signal(barrier, inc=1, device_id=(seq_id(d), head), device_id_type=MESH)
    for d in range(1, n_out):
        pl.semaphore_signal(barrier, inc=1, device_id=(me, z_id(d) * 2 + y), device_id_type=MESH)
    pl.semaphore_signal(barrier, inc=1, device_id=(me, mate), device_id_type=MESH)
    pl.semaphore_wait(barrier, n_seq + n_out - 1)

    def remote(src, dst, ss, rs, device):
        return pltpu.make_async_remote_copy(
            src_ref=src, dst_ref=dst, send_sem=ss, recv_sem=rs, device_id=device, device_id_type=MESH
        )

    sends = []

    def send(src, dst, ss, rs, device):
        copy = remote(src, dst, ss, rs, device)
        copy.start()
        sends.append(copy)

    def arrive(dst, ss, rs, device):
        remote(dst, dst, ss, rs, device).wait_recv()

    for d in range(1, n_seq):
        p = seq_id(d)
        send(q_ref, q_all.at[me], q_s.at[p], q_r.at[me], (p, head))

    column = pl.multiple_of(head * heads // GQA * DH, DH)
    k_ref[:stripe] = ck_ref[:, pl.ds(column, DH)]
    k_ref[stripe:] = nk_ref[:, pl.ds(column, DH)]
    v_ref[:stripe] = cv_ref[:, pl.ds(column, DH)]
    v_ref[stripe:] = nv_ref[:, pl.ds(column, DH)]

    pos_row = pos_ref[...].astype(f32)

    def token_pos(b):
        pick = lax.broadcasted_iota(jnp.int32, (tok, total), 0) + b * tok
        lane = lax.broadcasted_iota(jnp.int32, (tok, total), 1)
        return jnp.sum(jnp.where(pick == lane, pos_row, 0.0), axis=1, keepdims=True)

    eye = lax.broadcasted_iota(jnp.int32, (tok, tok), 0) == lax.broadcasted_iota(
        jnp.int32, (tok, tok), 1
    )
    own_row = jnp.sum(jnp.where(eye, token_pos(me), 0.0), axis=0, keepdims=True)
    live = lax.broadcasted_iota(jnp.int32, (1, stripe), 1) < len_ref[me]
    key_row = jnp.concatenate([jnp.where(live, -1.0, 1e9), own_row], axis=1)
    scale = DH ** (-0.5)

    def attend(block, b):
        stacked = jnp.concatenate([block[:, h * DH : (h + 1) * DH] for h in range(heads)], axis=0)
        scores = lax.dot_general(
            stacked, k_ref[...], (((1,), (1,)), ((), ())), preferred_element_type=f32
        ) * scale
        shown = key_row <= token_pos(b)
        scores = jnp.concatenate(
            [
                jnp.where(shown, scores[h * tok : (h + 1) * tok], HIDDEN)
                for h in range(heads)
            ],
            axis=0,
        )
        peak = jnp.max(scores, axis=1, keepdims=True)
        expo = jnp.exp(scores - peak)
        weight = jnp.sum(expo, axis=1, keepdims=True)
        mixed = jnp.dot(expo.astype(bf16), v_ref[...], preferred_element_type=f32) / weight
        level = peak + jnp.log(weight)
        lane = lax.broadcasted_iota(jnp.int32, (tok, DH), 1)
        stats = jnp.zeros((tok, DH), f32)
        for h in range(heads):
            stats = jnp.where(lane == h, level[h * tok : (h + 1) * tok], stats)
        mixed = jnp.concatenate([mixed[h * tok : (h + 1) * tok] for h in range(heads)], axis=1)
        return mixed, stats

    own_mixed, own_stats = attend(q_ref[...], me)
    for d in range(1, n_seq):
        p = seq_id(d)
        arrive(q_all.at[p], q_s.at[p], q_r.at[p], (p, head))
        mixed, stats = attend(q_all[p], p)
        o_send[p] = mixed.astype(bf16)
        t_send[p] = stats
        send(t_send.at[p], t_recv.at[me], t_s.at[p], t_r.at[me], (p, head))
        send(o_send.at[p], o_recv.at[me], o_s.at[p], o_r.at[me], (p, head))

    for d in range(1, n_seq):
        p = seq_id(d)
        arrive(t_recv.at[p], t_s.at[p], t_r.at[p], (p, head))
    top = own_stats
    for d in range(1, n_seq):
        top = jnp.maximum(top, t_recv[seq_id(d)])

    def spread(share):
        return jnp.concatenate(
            [jnp.broadcast_to(share[:, h : h + 1], (tok, DH)) for h in range(heads)], axis=1
        )

    share = jnp.exp(own_stats - top)
    norm = share
    mixed = own_mixed * spread(share)
    for d in range(1, n_seq):
        p = seq_id(d)
        arrive(o_recv.at[p], o_s.at[p], o_r.at[p], (p, head))
        share = jnp.exp(t_recv[p] - top)
        norm = norm + share
        mixed = mixed + o_recv[p].astype(f32) * spread(share)
    att[me] = (mixed / spread(norm)).astype(bf16)

    for d in range(1, n_seq):
        p = seq_id(d)
        send(att.at[me], att.at[me], a_s.at[p], a_r.at[me], (p, head))
    for d in range(1, n_seq):
        p = seq_id(d)
        arrive(att.at[p], a_s.at[p], a_r.at[p], (p, head))
    w_copy.wait()

    def project(g, side):
        begin = pl.multiple_of(g * wide + side * half, 128)
        return jnp.dot(
            att[...].reshape(total, width), w_ref[:, pl.ds(begin, half)], preferred_element_type=f32
        )

    for g in range(groups):
        y_send[g] = project(g, 1 - y).astype(bf16)
        send(y_send.at[g], y_recv.at[g], y_s.at[g], y_r.at[g], (me, mate))
    for g in range(groups):
        mine = project(g, y)
        arrive(y_recv.at[g], y_s.at[g], y_r.at[g], (me, mate))
        summed = mine + y_recv[g].astype(f32)
        z_send[g] = summed.astype(bf16).reshape(n_out, rows, half)
        own[g] = summed.reshape(n_out, rows, half)
        for d in range(1, n_out):
            p = z_id(d)
            send(z_send.at[g, p], z_recv.at[g, z], z_s.at[g, p], z_r.at[g, z], (me, p * 2 + y))
    for g in range(groups):
        result = own[g, z]
        for d in range(1, n_out):
            p = z_id(d)
            arrive(z_recv.at[g, p], z_s.at[g, p], z_r.at[g, p], (me, p * 2 + y))
            result = result + z_recv[g, p].astype(f32)
        fin[g, y, z] = result.astype(bf16)
        for d in range(1, n_out):
            p = z_id(d)
            send(fin.at[g, y, z], fin.at[g, y, z], f_s.at[g, p], f_r.at[g, z], (me, p * 2 + y))
        send(fin.at[g, y, z], fin.at[g, y, z], g_s.at[g, z], g_r.at[g, z], (me, mate))

    def place(g, side, r):
        begin = pl.multiple_of(g * wide + side * half, 128)
        out_ref[pl.ds(pl.multiple_of(r * rows, rows), rows), pl.ds(begin, half)] = fin[g, side, r]

    for g in range(groups):
        place(g, y, z)
        for d in range(1, n_out):
            p = z_id(d)
            arrive(fin.at[g, y, p], f_s.at[g, p], f_r.at[g, p], (me, p * 2 + y))
            send(fin.at[g, y, p], fin.at[g, y, p], g_s.at[g, p], g_r.at[g, p], (me, mate))
            place(g, y, p)
    for g in range(groups):
        for d in range(n_out):
            p = z_id(d)
            arrive(fin.at[g, 1 - y, p], g_s.at[g, p], g_r.at[g, p], (me, mate))
            place(g, 1 - y, p)
    for copy in sends:
        copy.wait_send()


def body(n_seq, n_head, queries, new_keys, new_values, cache_keys, cache_values, positions, cache_len, out_weight):
    tok, width = queries.shape
    stripe = cache_keys.shape[0]
    depth, cols = out_weight.shape
    total = n_seq * tok
    n_out = n_head // 2
    groups = max(1, min(4, cols // 256))
    half = cols // groups // 2
    rows = total // n_out
    bf16, f32 = jnp.bfloat16, jnp.float32
    vmem = pl.BlockSpec(memory_space=pltpu.VMEM)
    dma = pltpu.SemaphoreType.DMA
    out = pl.pallas_call(
        partial(kernel, n_seq, n_head, groups),
        out_shape=jax.ShapeDtypeStruct((total, cols), bf16),
        in_specs=[vmem] * 6
        + [pl.BlockSpec(memory_space=pltpu.SMEM), pl.BlockSpec(memory_space=pl.ANY)],
        out_specs=vmem,
        scratch_shapes=[
            pltpu.VMEM((depth, cols), bf16),
            pltpu.VMEM((stripe + tok, DH), bf16),
            pltpu.VMEM((stripe + tok, DH), bf16),
            pltpu.VMEM((n_seq, tok, width), bf16),
            pltpu.VMEM((n_seq, tok, width), bf16),
            pltpu.VMEM((n_seq, tok, width), bf16),
            pltpu.VMEM((n_seq, tok, DH), f32),
            pltpu.VMEM((n_seq, tok, DH), f32),
            pltpu.VMEM((n_seq, tok, width), bf16),
            pltpu.VMEM((groups, total, half), bf16),
            pltpu.VMEM((groups, total, half), bf16),
            pltpu.VMEM((groups, n_out, rows, half), bf16),
            pltpu.VMEM((groups, n_out, rows, half), bf16),
            pltpu.VMEM((groups, n_out, rows, half), f32),
            pltpu.VMEM((groups, 2, n_out, rows, half), bf16),
            dma,
        ]
        + [dma((n_seq,))] * 8
        + [dma((groups,))] * 2
        + [dma((groups, n_out))] * 6,
        compiler_params=pltpu.CompilerParams(
            collective_id=0, has_side_effects=True, vmem_limit_bytes=48 * 1024 * 1024
        ),
    )(
        queries, cache_keys, new_keys, cache_values, new_values,
        positions.reshape(1, total), cache_len, out_weight,
    )
    return out.astype(f32)


def solution(mesh):
    placed = (
        P("seq", "head"),
        P("seq", None),
        P("seq", None),
        P("seq", None),
        P("seq", None),
        P(),
        P(),
        P("head", "seq"),
    )
    return jax.shard_map(
        partial(body, mesh.shape["seq"], mesh.shape["head"]),
        mesh=mesh, in_specs=placed, out_specs=P(None, "seq"), check_vma=False,
    )
```

```python
from functools import partial

import jax
import jax.numpy as jnp
from jax import lax
from jax.experimental import pallas as pl
from jax.experimental.pallas import tpu as pltpu
from jax.sharding import PartitionSpec as P

DH = 128
GQA = 16
MESH = pl.DeviceIdType.MESH
HIDDEN = -1e30


def kernel(
    n_seq, n_head, groups, first,
    q_hbm, ck_hbm, nk_hbm, cv_hbm, nv_hbm, pos_hbm, len_hbm, w_hbm,
    out_ref,
    q_ref, pos_ref, len_ref, w_ref, k_ref, v_ref,
    q_all, o_send, o_recv, t_send, t_recv, att,
    y_send, y_recv, own, up_send, up_recv, down_send, down_recv, fin, x_send, x_recv,
    w_sem, in_sem, q_s, q_r, o_s, o_r, t_s, t_r, a_s, a_r,
    y_s, y_r, up_s, up_r, down_s, down_r, fup_s, fdown_s, f_r, g_s, g_r, x_s, x_r, h_s, h_r,
):
    f32, bf16 = jnp.float32, jnp.bfloat16
    me = lax.axis_index("seq")
    head = lax.axis_index("head")
    n_out = n_head // 2
    y = lax.rem(head, 2)
    z = head // 2
    mate = z * 2 + (1 - y)
    tok, width = q_ref.shape
    heads = width // DH
    stripe = ck_hbm.shape[0]
    total = n_seq * tok
    cols = w_hbm.shape[1]
    wide = cols // groups
    half = wide // 2
    rows = total // n_out

    column = pl.multiple_of(head * heads // GQA * DH, DH)
    loads = [
        pltpu.make_async_copy(src, dst, in_sem.at[i])
        for i, (src, dst) in enumerate(
            (
                (q_hbm, q_ref),
                (pos_hbm, pos_ref),
                (len_hbm, len_ref),
                (ck_hbm.at[:, pl.ds(column, DH)], k_ref.at[pl.ds(0, stripe)]),
                (nk_hbm.at[:, pl.ds(column, DH)], k_ref.at[pl.ds(stripe, tok)]),
                (cv_hbm.at[:, pl.ds(column, DH)], v_ref.at[pl.ds(0, stripe)]),
                (nv_hbm.at[:, pl.ds(column, DH)], v_ref.at[pl.ds(stripe, tok)]),
            )
        )
    ]
    for copy in loads:
        copy.start()
    w_copy = pltpu.make_async_copy(w_hbm, w_ref, w_sem)
    w_copy.start()

    def seq_id(d):
        return lax.rem(me + d, n_seq)

    def z_id(d):
        return lax.rem(z + d, n_out)

    barrier = pltpu.get_barrier_semaphore()
    for d in range(1, n_seq):
        pl.semaphore_signal(barrier, inc=1, device_id=(seq_id(d), head), device_id_type=MESH)
    above = lax.rem(z + 1, n_out) * 2 + y
    below = lax.rem(z + n_out - 1, n_out) * 2 + y
    pl.semaphore_signal(barrier, inc=1, device_id=(me, mate), device_id_type=MESH)

    @pl.when(z < n_out - 1)
    def _():
        pl.semaphore_signal(barrier, inc=1, device_id=(me, above), device_id_type=MESH)

    @pl.when(z > 0)
    def _():
        pl.semaphore_signal(barrier, inc=1, device_id=(me, below), device_id_type=MESH)

    inner = jnp.where(z > 0, 1, 0) + jnp.where(z < n_out - 1, 1, 0)
    pl.semaphore_wait(barrier, n_seq + inner)

    def remote(src, dst, ss, rs, device):
        return pltpu.make_async_remote_copy(
            src_ref=src, dst_ref=dst, send_sem=ss, recv_sem=rs, device_id=device, device_id_type=MESH
        )

    sends = []

    def post(make, when=None):
        make().start()
        sends.append((make, when))

    def send(src, dst, ss, rs, device):
        post(lambda: remote(src, dst, ss, rs, device))

    def arrive(dst, ss, rs, device):
        remote(dst, dst, ss, rs, device).wait_recv()

    loads[0].wait()
    for d in range(1, n_seq):
        p = seq_id(d)
        send(q_ref, q_all.at[me], q_s.at[p], q_r.at[me], (p, head))

    for copy in loads[1:]:
        copy.wait()
    pos_row = pos_ref[...].astype(f32)

    def token_pos(b):
        pick = lax.broadcasted_iota(jnp.int32, (tok, total), 0) + b * tok
        lane = lax.broadcasted_iota(jnp.int32, (tok, total), 1)
        return jnp.sum(jnp.where(pick == lane, pos_row, 0.0), axis=1, keepdims=True)

    eye = lax.broadcasted_iota(jnp.int32, (tok, tok), 0) == lax.broadcasted_iota(
        jnp.int32, (tok, tok), 1
    )
    own_row = jnp.sum(jnp.where(eye, token_pos(me), 0.0), axis=0, keepdims=True)
    live = lax.broadcasted_iota(jnp.int32, (1, stripe), 1) < len_ref[me]
    key_row = jnp.concatenate([jnp.where(live, -1.0, 1e9), own_row], axis=1)
    scale = DH ** (-0.5)

    def attend(block, b):
        stacked = jnp.concatenate([block[:, h * DH : (h + 1) * DH] for h in range(heads)], axis=0)
        scores = lax.dot_general(
            stacked, k_ref[...], (((1,), (1,)), ((), ())), preferred_element_type=f32
        ) * scale
        shown = key_row <= token_pos(b)
        scores = jnp.concatenate(
            [
                jnp.where(shown, scores[h * tok : (h + 1) * tok], HIDDEN)
                for h in range(heads)
            ],
            axis=0,
        )
        peak = jnp.max(scores, axis=1, keepdims=True)
        expo = jnp.exp(scores - peak)
        weight = jnp.sum(expo, axis=1, keepdims=True)
        mixed = jnp.dot(expo.astype(bf16), v_ref[...], preferred_element_type=f32) / weight
        level = peak + jnp.log(weight)
        lane = lax.broadcasted_iota(jnp.int32, (tok, DH), 1)
        stats = jnp.zeros((tok, DH), f32)
        for h in range(heads):
            stats = jnp.where(lane == h, level[h * tok : (h + 1) * tok], stats)
        mixed = jnp.concatenate([mixed[h * tok : (h + 1) * tok] for h in range(heads)], axis=1)
        return mixed, stats

    own_mixed, own_stats = attend(q_ref[...], me)
    for d in range(1, n_seq):
        p = seq_id(d)
        arrive(q_all.at[p], q_s.at[p], q_r.at[p], (p, head))
        mixed, stats = attend(q_all[p], p)
        o_send[p] = mixed.astype(bf16)
        t_send[p] = stats
        send(t_send.at[p], t_recv.at[me], t_s.at[p], t_r.at[me], (p, head))
        send(o_send.at[p], o_recv.at[me], o_s.at[p], o_r.at[me], (p, head))

    for d in range(1, n_seq):
        p = seq_id(d)
        arrive(t_recv.at[p], t_s.at[p], t_r.at[p], (p, head))
    top = own_stats
    for d in range(1, n_seq):
        top = jnp.maximum(top, t_recv[seq_id(d)])

    def spread(share):
        return jnp.concatenate(
            [jnp.broadcast_to(share[:, h : h + 1], (tok, DH)) for h in range(heads)], axis=1
        )

    share = jnp.exp(own_stats - top)
    norm = share
    mixed = own_mixed * spread(share)
    for d in range(1, n_seq):
        p = seq_id(d)
        arrive(o_recv.at[p], o_s.at[p], o_r.at[p], (p, head))
        share = jnp.exp(t_recv[p] - top)
        norm = norm + share
        mixed = mixed + o_recv[p].astype(f32) * spread(share)
    att[me] = (mixed / spread(norm)).astype(bf16)

    for d in range(1, n_seq):
        p = seq_id(d)
        send(att.at[me], att.at[me], a_s.at[p], a_r.at[me], (p, head))
    for d in range(1, n_seq):
        p = seq_id(d)
        arrive(att.at[p], a_s.at[p], a_r.at[p], (p, head))
    w_copy.wait()

    def project(g, side):
        begin = pl.multiple_of(g * wide + side * half, 128)
        return jnp.dot(
            att[...].reshape(total, width), w_ref[:, pl.ds(begin, half)], preferred_element_type=f32
        )

    def place(g, side, r):
        begin = pl.multiple_of(g * wide + side * half, 128)
        out_ref[pl.ds(pl.multiple_of(r * rows, rows), rows), pl.ds(begin, half)] = fin[g, r, side]

    def reduce_step(j, t):
        rest = n_out - 1 - t

        @pl.when(z == t)
        def _():
            if t > 0:
                arrive(up_recv.at[j, pl.ds(t, rest + 1)], up_s.at[j], up_r.at[j], (me, below))
                own[j, t] = own[j, t] + up_recv[j, t].astype(f32)
            if rest > 0:
                part = own[j, t + 1 :]
                if t > 0:
                    part = part + up_recv[j, t + 1 :].astype(f32)
                up_send[j, t + 1 :] = part.astype(bf16)
                span = pl.ds(t + 1, rest)
                post(
                    lambda: remote(
                        up_send.at[j, span], up_recv.at[j, span], up_s.at[j], up_r.at[j], (me, above)
                    ),
                    lambda: z == t,
                )

        @pl.when(z == rest)
        def _():
            if t > 0:
                arrive(
                    down_recv.at[j, pl.ds(0, rest + 1)], down_s.at[j], down_r.at[j], (me, above)
                )
                own[j, rest] = own[j, rest] + down_recv[j, rest].astype(f32)
            if rest > 0:
                part = own[j, :rest]
                if t > 0:
                    part = part + down_recv[j, :rest].astype(f32)
                down_send[j, :rest] = part.astype(bf16)
                span = pl.ds(0, rest)
                post(
                    lambda: remote(
                        down_send.at[j, span], down_recv.at[j, span], down_s.at[j], down_r.at[j],
                        (me, below),
                    ),
                    lambda: z == rest,
                )

    def pass_up(g, j, side, p, when):
        def make():
            piece = fin.at[g, p, side]
            return remote(piece, piece, fup_s.at[j, p], f_r.at[j, p], (me, above))

        pl.when(when())(lambda: post(make, when))

    def pass_down(g, j, side, p, when):
        def make():
            piece = fin.at[g, p, side]
            return remote(piece, piece, fdown_s.at[j, p], f_r.at[j, p], (me, below))

        pl.when(when())(lambda: post(make, when))

    def to_mate(g, p, when=None):
        def make():
            piece = fin.at[g, p, y]
            return remote(piece, piece, g_s.at[g, p], g_r.at[g, p], (me, mate))

        post(make, when)

    def gather_step(g, j, side, t, mated):
        low, high = z - t, z + t

        @pl.when(low >= 0)
        def _():
            arrive(fin.at[g, low, side], fup_s.at[j, low], f_r.at[j, low], (me, below))
            pass_up(g, j, side, low, lambda: jnp.logical_and(low >= 0, z < n_out - 1))
            if mated:
                to_mate(g, low, lambda: low >= 0)
            place(g, side, low)

        @pl.when(high < n_out)
        def _():
            arrive(fin.at[g, high, side], fdown_s.at[j, high], f_r.at[j, high], (me, above))
            pass_down(g, j, side, high, lambda: jnp.logical_and(high < n_out, z > 0))
            if mated:
                to_mate(g, high, lambda: high < n_out)
            place(g, side, high)

    def open_gather(g, j, side):
        pass_up(g, j, side, z, lambda: z < n_out - 1)
        pass_down(g, j, side, z, lambda: z > 0)

    def pair_steps(g):
        j = g + first

        def begin():
            summed = project(g, y)
            arrive(y_recv.at[g], y_s.at[g], y_r.at[g], (me, mate))
            own[j] = (summed + y_recv[g].astype(f32)).reshape(n_out, rows, half)
            reduce_step(j, 0)

        def turn():
            reduce_step(j, n_out - 1)
            fin[g, z, y] = own[j, z].astype(bf16)
            open_gather(g, j, y)
            to_mate(g, z)
            place(g, y, z)

        def end():
            for d in range(n_out):
                p = z_id(d)
                arrive(fin.at[g, p, 1 - y], g_s.at[g, p], g_r.at[g, p], (me, mate))
                place(g, 1 - y, p)

        return (
            [begin]
            + [partial(reduce_step, j, t) for t in range(1, n_out - 1)]
            + [turn]
            + [partial(gather_step, g, j, y, t, True) for t in range(1, n_out)]
            + [end]
        )

    def line_steps():
        def begin():
            for side in range(2):
                own[side] = project(0, side).reshape(n_out, rows, half)
                reduce_step(side, 0)

        def reduce(t):
            for side in range(2):
                reduce_step(side, t)

        def swap():
            reduce(n_out - 1)
            x_send[...] = own[1 - y, z].astype(bf16)
            send(x_send, x_recv, x_s, x_r, (me, mate))

        def settle():
            arrive(x_recv, x_s, x_r, (me, mate))
            fin[0, z, y] = (own[y, z] + x_recv[...].astype(f32)).astype(bf16)
            piece = fin.at[0, z, y]
            send(piece, piece, h_s, h_r, (me, mate))
            open_gather(0, y, y)

        def turn():
            arrive(fin.at[0, z, 1 - y], h_s, h_r, (me, mate))
            open_gather(0, 1 - y, 1 - y)
            for side in range(2):
                place(0, side, z)

        def gather(t):
            for side in range(2):
                gather_step(0, side, side, t, False)

        return (
            [begin]
            + [partial(reduce, t) for t in range(1, n_out - 1)]
            + [swap, settle, turn]
            + [partial(gather, t) for t in range(1, n_out)]
        )

    for g in range(first, groups):
        y_send[g] = project(g, 1 - y).astype(bf16)
        send(y_send.at[g], y_recv.at[g], y_s.at[g], y_r.at[g], (me, mate))
    lines = ([line_steps()] if first else []) + [pair_steps(g) for g in range(first, groups)]
    for slot in range(max(i + len(steps) for i, steps in enumerate(lines))):
        for i, steps in enumerate(lines):
            if 0 <= slot - i < len(steps):
                steps[slot - i]()
    for make, when in sends:
        if when is None:
            make().wait_send()
        else:
            pl.when(when())(lambda: make().wait_send())


def body(n_seq, n_head, queries, new_keys, new_values, cache_keys, cache_values, positions, cache_len, out_weight):
    tok, width = queries.shape
    stripe = cache_keys.shape[0]
    depth, cols = out_weight.shape
    total = n_seq * tok
    n_out = n_head // 2
    groups = max(1, min(4, cols // 256))
    half = cols // groups // 2
    rows = total // n_out
    bf16, f32 = jnp.bfloat16, jnp.float32
    first = 1 if groups > 1 else 0
    chains = groups + first
    vmem = pl.BlockSpec(memory_space=pltpu.VMEM)
    dma = pltpu.SemaphoreType.DMA
    out = pl.pallas_call(
        partial(kernel, n_seq, n_head, groups, first),
        out_shape=jax.ShapeDtypeStruct((total, cols), bf16),
        in_specs=[pl.BlockSpec(memory_space=pl.ANY)] * 8,
        out_specs=vmem,
        scratch_shapes=[
            pltpu.VMEM((tok, width), bf16),
            pltpu.VMEM((1, total), jnp.int32),
            pltpu.SMEM(cache_len.shape, jnp.int32),
            pltpu.VMEM((depth, cols), bf16),
            pltpu.VMEM((stripe + tok, DH), bf16),
            pltpu.VMEM((stripe + tok, DH), bf16),
            pltpu.VMEM((n_seq, tok, width), bf16),
            pltpu.VMEM((n_seq, tok, width), bf16),
            pltpu.VMEM((n_seq, tok, width), bf16),
            pltpu.VMEM((n_seq, tok, DH), f32),
            pltpu.VMEM((n_seq, tok, DH), f32),
            pltpu.VMEM((n_seq, tok, width), bf16),
            pltpu.VMEM((groups, total, half), bf16),
            pltpu.VMEM((groups, total, half), bf16),
            pltpu.VMEM((chains, n_out, rows, half), f32),
        ]
        + [pltpu.VMEM((chains, n_out, rows, half), bf16)] * 4
        + [
            pltpu.VMEM((groups, n_out, 2, rows, half), bf16),
            pltpu.VMEM((rows, half), bf16),
            pltpu.VMEM((rows, half), bf16),
            dma,
            dma((7,)),
        ]
        + [dma((n_seq,))] * 8
        + [dma((groups,))] * 2
        + [dma((chains,))] * 4
        + [dma((chains, n_out))] * 3
        + [dma((groups, n_out))] * 2
        + [dma] * 4,
        compiler_params=pltpu.CompilerParams(
            collective_id=0, has_side_effects=True, vmem_limit_bytes=60 * 1024 * 1024
        ),
    )(
        queries, cache_keys, new_keys, cache_values, new_values,
        positions.reshape(1, total), cache_len, out_weight,
    )
    return out.astype(f32)


def solution(mesh):
    placed = (
        P("seq", "head"),
        P("seq", None),
        P("seq", None),
        P("seq", None),
        P("seq", None),
        P(),
        P(),
        P("head", "seq"),
    )
    return jax.shard_map(
        partial(body, mesh.shape["seq"], mesh.shape["head"]),
        mesh=mesh, in_specs=placed, out_specs=P(None, "seq"), check_vma=False,
    )
```
